32 devices in a mesh: zero: 4 (over z), model: 4 (over x, core), trial: 2 (over y).
Axes of the slice: x: 2, y: 2, z: 4, core: 2. Of those that a mesh axis runs over, the one named last changes fastest.
Arguments:
- w_query: bfloat16 [4096, 2048], P(('trial', 'zero'), 'model'), parts along dimension 0, may hold values from -0.125 to 0.125
- low_query: bfloat16 [4096, 32], P(('trial', 'zero')), parts along dimension 0, may hold values from -0.125 to 0.125
- high_query: bfloat16 [64, 2048], P('trial', 'model'), parts along dimension 0, may hold values from -1 to 1
- w_key: bfloat16 [4096, 512], P(('trial', 'zero'), 'model'), parts along dimension 0, may hold values from -0.125 to 0.125
- low_key: bfloat16 [4096, 32], P(('trial', 'zero')), parts along dimension 0, may hold values from -0.125 to 0.125
- high_key: bfloat16 [64, 512], P('trial', 'model'), parts along dimension 0, may hold values from -1 to 1
- w_value: bfloat16 [4096, 512], P(('trial', 'zero'), 'model'), parts along dimension 0, may hold values from -0.125 to 0.125
- low_value: bfloat16 [4096, 32], P(('trial', 'zero')), parts along dimension 0, may hold values from -0.125 to 0.125
- high_value: bfloat16 [64, 512], P('trial', 'model'), parts along dimension 0, may hold values from -1 to 1
- w_mixed: bfloat16 [4096, 2048], P(('trial', 'model'), 'zero'), parts along dimension 0, may hold values from -0.125 to 0.125
- low_mixed: bfloat16 [4096, 32], P(('trial', 'model')), parts along dimension 0, may hold values from -0.125 to 0.125
- high_mixed: bfloat16 [64, 2048], P('trial', 'zero'), parts along dimension 0, may hold values from -1 to 1
- norm_train: float32 [4096], P(('trial', 'zero', 'model')), parts along dimension 0, may hold values from 0.25 to 1.75
- norm_step: float32 [4096], P(('trial', 'zero', 'model')), parts along dimension 0, may hold values from -0.3 to 0.3
Outputs:
- final_query: bfloat16 [4096, 2048], P('trial', 'model'), parts along dimension 0
- final_key: bfloat16 [4096, 512], P('trial', 'model'), parts along dimension 0
- final_value: bfloat16 [4096, 512], P('trial', 'model'), parts along dimension 0
- final_mixed: bfloat16 [4096, 2048], P(('trial', 'model')), parts along dimension 0
- serve_norm: bfloat16 [4096], P('trial'), parts along dimension 0
The draws below stay inside these ranges and needn't reach their ends.
There are 2 independent parts, one for each index of `trial`. The reference program is written for one: setup_inputs(seed, part) draws one part's arguments, and reference() takes and returns one part's arrays. A program takes and returns all parts, laid end to end along the dimension named above; each array names one. Nothing has to cross between parts.
All inputs are finite; a program needn't handle non-finite values.
Results may differ from the reference program's by a relative error of at most 0.001.
Values may be sent and summed in bfloat16 or wider, within the bound.
A program may use at most 64 MiB of HBM per device.

```python
import jax
import jax.numpy as jnp

D_MODEL = 2048
Q_DIM = 2048
KV_DIM = 512
RANK = 32


def block_levels(stream_key, shape, shards, low, largest):
    loudness, own = 1.0, jax.random.fold_in(stream_key, 6)
    for position, shards_of in shards:
        draws = jnp.exp(jax.random.uniform(jax.random.fold_in(own, position), (shards_of,), jnp.float32, low / len(shards), largest / len(shards)))
        loudness = loudness * jnp.repeat(draws, shape[position] // shards_of).reshape([-1 if axis == position else 1 for axis in range(len(shape))])
    return loudness


def scatter_about(rng, extent, width, most, shards=(), dtype=jnp.bfloat16):
    result = jax.random.normal(rng, extent, jnp.float32) * width
    if len(shards) > 0:
        result = block_levels(rng, extent, shards, -0.22, 0.18) * result
    return jnp.clip(result, min=-most, max=most).astype(dtype)


def setup_inputs(seed: int = 0, part: int = 0) -> dict:
    splits = jax.random.split(jax.random.key(seed), 15)
    part_splits = jax.random.split(jax.random.fold_in(splits[14], part), 15)
    return {
        "w_query": scatter_about(part_splits[0], (D_MODEL, Q_DIM), D_MODEL ** -0.5, 0.125, ((0, 4), (1, 4))),
        "low_query": scatter_about(part_splits[1], (D_MODEL, RANK), D_MODEL ** -0.5, 0.125, ((0, 4),)),
        "high_query": scatter_about(part_splits[2], (RANK, Q_DIM), RANK ** -0.5, 1.0, ((1, 4),)),
        "w_key": scatter_about(part_splits[3], (D_MODEL, KV_DIM), D_MODEL ** -0.5, 0.125, ((0, 4), (1, 4))),
        "low_key": scatter_about(part_splits[4], (D_MODEL, RANK), D_MODEL ** -0.5, 0.125, ((0, 4),)),
        "high_key": scatter_about(part_splits[5], (RANK, KV_DIM), RANK ** -0.5, 1.0, ((1, 4),)),
        "w_value": scatter_about(part_splits[6], (D_MODEL, KV_DIM), D_MODEL ** -0.5, 0.125, ((0, 4), (1, 4))),
        "low_value": scatter_about(part_splits[7], (D_MODEL, RANK), D_MODEL ** -0.5, 0.125, ((0, 4),)),
        "high_value": scatter_about(part_splits[8], (RANK, KV_DIM), RANK ** -0.5, 1.0, ((1, 4),)),
        "w_mixed": scatter_about(part_splits[9], (Q_DIM, D_MODEL), Q_DIM ** -0.5, 0.125, ((0, 4), (1, 4))),
        "low_mixed": scatter_about(part_splits[10], (Q_DIM, RANK), Q_DIM ** -0.5, 0.125, ((0, 4),)),
        "high_mixed": scatter_about(part_splits[11], (RANK, D_MODEL), RANK ** -0.5, 1.0, ((1, 4),)),
        "norm_train": jnp.clip(1.0 + 0.15 * jax.random.normal(part_splits[12], (D_MODEL,), jnp.float32), 0.25, 1.75),
        "norm_step": jnp.clip(jax.random.uniform(part_splits[13], (D_MODEL,), jnp.float32, -0.3, 0.3) * block_levels(part_splits[13], (D_MODEL,), ((0, 16),), -0.4, 0.0), -0.3, 0.3),
    }


mix_rate = 2.0


def reference(w_query, low_query, high_query, w_key, low_key, high_key, w_value, low_value, high_value, w_mixed, low_mixed, high_mixed, norm_train, norm_step):
    result_query = w_query.astype(jnp.float32) + mix_rate * jnp.dot(low_query, high_query, preferred_element_type=jnp.float32)
    result_key = w_key.astype(jnp.float32) + mix_rate * jnp.dot(low_key, high_key, preferred_element_type=jnp.float32)
    result_value = w_value.astype(jnp.float32) + mix_rate * jnp.dot(low_value, high_value, preferred_element_type=jnp.float32)
    result_mixed = w_mixed.astype(jnp.float32) + mix_rate * jnp.dot(low_mixed, high_mixed, preferred_element_type=jnp.float32)
    final_query = result_query.astype(jnp.bfloat16)
    final_key = result_key.astype(jnp.bfloat16)
    final_value = result_value.astype(jnp.bfloat16)
    final_mixed = result_mixed.astype(jnp.bfloat16)
    serve_norm = (norm_train + norm_step).astype(jnp.bfloat16)
    return final_query, final_key, final_value, final_mixed, serve_norm
```

```python
import functools

import jax
import jax.numpy as jnp
from jax import lax
from jax.experimental import pallas as pl
from jax.experimental.pallas import tpu as pltpu
from jax.sharding import PartitionSpec as P

MESH = pl.DeviceIdType.MESH
mix_rate = 2.0
piece_rows = 128


def merge_and_gather(zeros, models, *refs):
    (w_q, low_q, high_q, w_k, low_k, high_k, w_v, low_v, high_v, w_m, low_m, high_m) = refs[:12]
    train, step = refs[12:14]
    out_q, out_k, out_v, out_m, out_n = refs[14:19]
    held = refs[19:33]
    load_sem, send_sem, recv_sem, row_send, row_recv = refs[33:]

    z = lax.axis_index("zero")
    m = lax.axis_index("model")
    has_right, has_left = z < zeros - 1, z > 0

    loads = []
    for i in (1, 2, 0, 12, 13, 4, 5, 3, 7, 8, 6, 10, 11, 9):
        copy = pltpu.make_async_copy(refs[i], held[i], load_sem.at[i])
        copy.start()
        loads.append((i, copy))
    loads = dict(loads)

    barrier = pltpu.get_barrier_semaphore()

    @pl.when(has_right)
    def _():
        pl.semaphore_signal(barrier, inc=1, device_id={"zero": z + 1}, device_id_type=MESH)

    @pl.when(has_left)
    def _():
        pl.semaphore_signal(barrier, inc=1, device_id={"zero": z - 1}, device_id_type=MESH)

    for d in range(1, models):
        pl.semaphore_signal(
            barrier, inc=1, device_id={"model": lax.rem(m + d, models)}, device_id_type=MESH
        )

    pieces = []

    def rows_of(out, w):
        rows = w.shape[0]
        size = min(piece_rows, rows)
        return [(out, w, first, size) for first in range(0, rows, size)]

    groups = []
    for position, (out, w) in enumerate(((out_q, w_q), (out_k, w_k), (out_v, w_v), (out_m, w_m))):
        own = rows_of(out, w)
        groups.append((position, len(pieces), own))
        pieces += own
    count = len(pieces) + 1

    def view(shard, c):
        if c == count - 1:
            return out_n.at[shard]
        out, w, first, size = pieces[c]
        rows, columns = w.shape
        if out is out_m:
            return out.at[pl.ds(first, size), pl.ds(pl.multiple_of(shard * columns, columns), columns)]
        return out.at[pl.ds(pl.multiple_of(shard * rows + first, size), size), :]

    def hop(shard, c, way):
        return pltpu.make_async_remote_copy(
            src_ref=view(shard, c),
            dst_ref=view(shard, c),
            send_sem=send_sem.at[way, shard, c],
            recv_sem=recv_sem.at[shard, c],
            device_id={"zero": z + 1 if way == 0 else z - 1},
            device_id_type=MESH,
        )

    def send_own(c):
        @pl.when(has_right)
        def _():
            hop(z, c, 0).start()

        @pl.when(has_left)
        def _():
            hop(z, c, 1).start()

    ready = []
    waited = False
    for position, base, own in groups:
        for i in (1, 2, 0):
            loads[3 * position + i].wait()
        w, low, high = held[3 * position : 3 * position + 3]
        for j, (out, _, first, size) in enumerate(own):
            product = lax.dot_general(
                low[:, first : first + size],
                high[...],
                (((0,), (0,)), ((), ())),
                preferred_element_type=jnp.float32,
            )
            merged = w[first : first + size, :].astype(jnp.float32) + mix_rate * product
            view(z, base + j)[...] = merged.astype(out.dtype)
            ready.append(base + j)
        if position == 0:
            loads[12].wait()
            loads[13].wait()
            out_n[z, m] = held[12][...] + held[13][...]
            pl.semaphore_wait(
                barrier, models - 1 + has_right.astype(jnp.int32) + has_left.astype(jnp.int32)
            )
        while len(ready) > 1:
            send_own(ready.pop(0))
    send_own(ready.pop(0))

    def row(d):
        return pltpu.make_async_remote_copy(
            src_ref=out_n.at[z, m],
            dst_ref=out_n.at[z, m],
            send_sem=row_send.at[d],
            recv_sem=row_recv.at[d],
            device_id={"model": lax.rem(m + d, models)},
            device_id_type=MESH,
        )

    def row_from(d):
        sender = lax.rem(m + models - d, models)
        return pltpu.make_async_remote_copy(
            src_ref=out_n.at[z, sender],
            dst_ref=out_n.at[z, sender],
            send_sem=row_send.at[d],
            recv_sem=row_recv.at[d],
            device_id={"model": sender},
            device_id_type=MESH,
        )

    for d in range(1, models):
        row(d).start()
    for d in range(1, models):
        row_from(d).wait_recv()
    send_own(count - 1)

    def pass_on(k, carry):
        from_left, from_right = z - 1 - k, z + 1 + k
        for c in range(count):

            @pl.when(from_left >= 0)
            def _():
                hop(from_left, c, 0).wait_recv()

                @pl.when(has_right)
                def _():
                    hop(from_left, c, 0).start()

            @pl.when(from_right < zeros)
            def _():
                hop(from_right, c, 1).wait_recv()

                @pl.when(has_left)
                def _():
                    hop(from_right, c, 1).start()

        return carry

    lax.fori_loop(0, zeros - 1, pass_on, 0)

    for d in range(1, models):
        row(d).wait_send()

    def drain(k, carry):
        for c in range(count):

            @pl.when(jnp.logical_and(has_right, z - k >= 0))
            def _():
                hop(z - k, c, 0).wait_send()

            @pl.when(jnp.logical_and(has_left, z + k < zeros))
            def _():
                hop(z + k, c, 1).wait_send()

        return carry

    lax.fori_loop(0, zeros, drain, 0)


def shards(zeros, models, *args):
    args = list(args)
    for i in (1, 4, 7, 10):
        args[i] = args[i].T
    for i in (12, 13):
        args[i] = args[i].reshape(1, -1)
    w_q, w_k, w_v, w_m = args[0], args[3], args[6], args[9]
    count = sum(-(-w.shape[0] // min(piece_rows, w.shape[0])) for w in (w_q, w_k, w_v, w_m)) + 1
    outs = [pltpu.VMEM((zeros * w.shape[0], w.shape[1]), w.dtype) for w in (w_q, w_k, w_v)]
    outs.append(pltpu.VMEM((w_m.shape[0], zeros * w_m.shape[1]), w_m.dtype))
    outs.append(pltpu.VMEM((zeros, models, 1, args[12].shape[1]), jnp.float32))
    final_query, final_key, final_value, final_mixed, norm = pl.pallas_call(
        functools.partial(merge_and_gather, zeros, models),
        out_shape=[jax.ShapeDtypeStruct(o.shape, o.dtype) for o in outs],
        in_specs=[pl.BlockSpec(memory_space=pl.ANY)] * 14,
        out_specs=[pl.BlockSpec(memory_space=pltpu.VMEM)] * 5,
        scratch_shapes=[pltpu.VMEM(a.shape, a.dtype) for a in args]
        + [
            pltpu.SemaphoreType.DMA((14,)),
            pltpu.SemaphoreType.DMA((2, zeros, count)),
            pltpu.SemaphoreType.DMA((zeros, count)),
            pltpu.SemaphoreType.DMA((models,)),
            pltpu.SemaphoreType.DMA((models,)),
        ],
        compiler_params=pltpu.CompilerParams(collective_id=0, has_side_effects=True),
    )(*args)
    serve_norm = norm.reshape(-1).astype(jnp.bfloat16)
    return final_query, final_key, final_value, final_mixed, serve_norm


def solution(mesh):
    placed = (
        P(("trial", "zero"), "model"),
        P(("trial", "zero"), None),
        P("trial", "model"),
        P(("trial", "zero"), "model"),
        P(("trial", "zero"), None),
        P("trial", "model"),
        P(("trial", "zero"), "model"),
        P(("trial", "zero"), None),
        P("trial", "model"),
        P(("trial", "model"), "zero"),
        P(("trial", "model"), None),
        P("trial", "zero"),
        P(("trial", "zero", "model")),
        P(("trial", "zero", "model")),
    )
    return jax.shard_map(
        functools.partial(shards, mesh.shape["zero"], mesh.shape["model"]),
        mesh=mesh,
        in_specs=placed,
        out_specs=(
            P("trial", "model"),
            P("trial", "model"),
            P("trial", "model"),
            P(("trial", "model"), None),
            P("trial"),
        ),
        check_vma=False,
    )
```

```python
import functools
import math

import jax
import jax.numpy as jnp
from jax import lax
from jax.experimental import pallas as pl
from jax.experimental.pallas import tpu as pltpu
from jax.sharding import PartitionSpec as P

MESH = pl.DeviceIdType.MESH
mix_rate = 2.0
piece_rows = 128
vmem_bytes = 67043328


def merge_and_gather(zeros, models, *refs):
    (w_q, low_q, high_q, w_k, low_k, high_k, w_v, low_v, high_v, w_m, low_m, high_m) = refs[:12]
    train, step = refs[12:14]
    out_q, out_k, out_v, out_m, out_n = refs[14:19]
    held = refs[19:33]
    load_sem, send_sem, recv_sem, row_send, row_recv = refs[33:]

    z = lax.axis_index("zero")
    m = lax.axis_index("model")
    has_right, has_left = z < zeros - 1, z > 0

    barrier = pltpu.get_barrier_semaphore()

    @pl.when(has_right)
    def _():
        pl.semaphore_signal(barrier, inc=1, device_id={"zero": z + 1}, device_id_type=MESH)

    @pl.when(has_left)
    def _():
        pl.semaphore_signal(barrier, inc=1, device_id={"zero": z - 1}, device_id_type=MESH)

    for d in range(1, models):
        pl.semaphore_signal(
            barrier, inc=1, device_id={"model": lax.rem(m + d, models)}, device_id_type=MESH
        )

    loads = []
    for i in (1, 2, 0, 12, 13, 4, 5, 3, 7, 8, 6, 10, 11, 9):
        copy = pltpu.make_async_copy(refs[i], held[i], load_sem.at[i])
        copy.start()
        loads.append((i, copy))
    loads = dict(loads)

    pieces = []

    def rows_of(out, w):
        rows = w.shape[0]
        size = min(piece_rows, rows)
        return [(out, w, first, size) for first in range(0, rows, size)]

    groups = []
    for position, (out, w) in enumerate(((out_q, w_q), (out_k, w_k), (out_v, w_v), (out_m, w_m))):
        own = rows_of(out, w)
        groups.append((position, len(pieces), own))
        pieces += own
    count = len(pieces) + 1

    def view(shard, c):
        if c == count - 1:
            return out_n.at[shard]
        out, w, first, size = pieces[c]
        rows, columns = w.shape
        if out is out_m:
            return out.at[pl.ds(first, size), pl.ds(pl.multiple_of(shard * columns, columns), columns)]
        return out.at[pl.ds(pl.multiple_of(shard * rows + first, size), size), :]

    def hop(shard, c, way):
        return pltpu.make_async_remote_copy(
            src_ref=view(shard, c),
            dst_ref=view(shard, c),
            send_sem=send_sem.at[way, shard, c],
            recv_sem=recv_sem.at[shard, c],
            device_id={"zero": z + 1 if way == 0 else z - 1},
            device_id_type=MESH,
        )

    def send_own(c):
        @pl.when(has_right)
        def _():
            hop(z, c, 0).start()

        @pl.when(has_left)
        def _():
            hop(z, c, 1).start()

    def row(d):
        return pltpu.make_async_remote_copy(
            src_ref=out_n.at[z, m],
            dst_ref=out_n.at[z, m],
            send_sem=row_send.at[d],
            recv_sem=row_recv.at[d],
            device_id={"model": lax.rem(m + d, models)},
            device_id_type=MESH,
        )

    def row_from(d):
        sender = lax.rem(m + models - d, models)
        return pltpu.make_async_remote_copy(
            src_ref=out_n.at[z, sender],
            dst_ref=out_n.at[z, sender],
            send_sem=row_send.at[d],
            recv_sem=row_recv.at[d],
            device_id={"model": sender},
            device_id_type=MESH,
        )

    ready = []
    for position, base, own in groups:
        for i in (1, 2, 0):
            loads[3 * position + i].wait()
        w, low, high = held[3 * position : 3 * position + 3]
        for j, (out, _, first, size) in enumerate(own):
            product = lax.dot_general(
                low[:, first : first + size],
                high[...],
                (((0,), (0,)), ((), ())),
                preferred_element_type=jnp.float32,
            )
            merged = w[first : first + size, :].astype(jnp.float32) + mix_rate * product
            view(z, base + j)[...] = merged.astype(out.dtype)
            ready.append(base + j)
            if len(ready) == 2:
                if ready[0] == 0:
                    pl.semaphore_wait(
                        barrier, models - 1 + has_right.astype(jnp.int32) + has_left.astype(jnp.int32)
                    )
                send_own(ready.pop(0))
        if position == 0:
            loads[12].wait()
            loads[13].wait()
            out_n[z, m] = held[12][...] + held[13][...]
    for d in range(1, models):
        row(d).start()
    send_own(ready.pop(0))
    for d in range(1, models):
        row_from(d).wait_recv()
    send_own(count - 1)

    def pass_on(k, carry):
        from_left, from_right = z - 1 - k, z + 1 + k
        for c in range(count):

            @pl.when(from_left >= 0)
            def _():
                hop(from_left, c, 0).wait_recv()

                @pl.when(has_right)
                def _():
                    hop(from_left, c, 0).start()

            @pl.when(from_right < zeros)
            def _():
                hop(from_right, c, 1).wait_recv()

                @pl.when(has_left)
                def _():
                    hop(from_right, c, 1).start()

        return carry

    lax.fori_loop(0, zeros - 1, pass_on, 0)

    for d in range(1, models):
        row(d).wait_send()

    def drain(k, carry):
        for c in range(count):

            @pl.when(jnp.logical_and(has_right, z - k >= 0))
            def _():
                hop(z - k, c, 0).wait_send()

            @pl.when(jnp.logical_and(has_left, z + k < zeros))
            def _():
                hop(z + k, c, 1).wait_send()

        return carry

    lax.fori_loop(0, zeros, drain, 0)


def write_out(*refs):
    norm, wide, narrow, sem = refs[4], refs[10], refs[11], refs[12]
    copies = [pltpu.make_async_copy(refs[i], refs[5 + i], sem.at[i]) for i in (0, 3, 1, 2)]
    for copy in copies:
        copy.start()
    models = norm.shape[1]
    for i in range(wide.shape[0]):
        wide[i : i + 1, :] = norm[i // models, i % models]
    narrow[...] = wide[...].astype(narrow.dtype)
    copies.append(pltpu.make_async_copy(narrow, refs[9], sem.at[4]))
    copies[-1].start()
    for copy in copies:
        copy.wait()


def shards(zeros, models, *args):
    args = list(args)
    for i in (1, 4, 7, 10):
        args[i] = args[i].T
    for i in (12, 13):
        args[i] = args[i].reshape(1, -1)
    w_q, w_k, w_v, w_m = args[0], args[3], args[6], args[9]
    count = sum(-(-w.shape[0] // min(piece_rows, w.shape[0])) for w in (w_q, w_k, w_v, w_m)) + 1
    outs = [pltpu.VMEM((zeros * w.shape[0], w.shape[1]), w.dtype) for w in (w_q, w_k, w_v)]
    outs.append(pltpu.VMEM((w_m.shape[0], zeros * w_m.shape[1]), w_m.dtype))
    outs.append(pltpu.VMEM((zeros, models, 1, args[12].shape[1]), jnp.float32))
    held_bytes = sum(math.prod(o.shape) * jnp.dtype(o.dtype).itemsize for o in outs)
    final_query, final_key, final_value, final_mixed, norm = pl.pallas_call(
        functools.partial(merge_and_gather, zeros, models),
        out_shape=outs,
        in_specs=[pl.BlockSpec(memory_space=pltpu.HBM)] * 14,
        scratch_shapes=[pltpu.VMEM(a.shape, a.dtype) for a in args]
        + [
            pltpu.SemaphoreType.DMA((14,)),
            pltpu.SemaphoreType.DMA((2, zeros, count)),
            pltpu.SemaphoreType.DMA((zeros, count)),
            pltpu.SemaphoreType.DMA((models,)),
            pltpu.SemaphoreType.DMA((models,)),
        ],
        compiler_params=pltpu.CompilerParams(
            collective_id=0,
            has_side_effects=True,
            vmem_limit_bytes=vmem_bytes - held_bytes - 128 * 1024,
        ),
    )(*args)
    gathered = [final_query, final_key, final_value, final_mixed]
    gains = norm.shape[0] * norm.shape[1], norm.shape[3]
    *finals, serve_norm = pl.pallas_call(
        write_out,
        out_shape=[jax.ShapeDtypeStruct(g.shape, g.dtype) for g in gathered]
        + [jax.ShapeDtypeStruct(gains, jnp.bfloat16)],
        in_specs=[pl.BlockSpec(memory_space=pltpu.VMEM)] * 5,
        out_specs=[pl.BlockSpec(memory_space=pltpu.HBM)] * 5,
        scratch_shapes=[
            pltpu.VMEM(gains, jnp.float32),
            pltpu.VMEM(gains, jnp.bfloat16),
            pltpu.SemaphoreType.DMA((5,)),
        ],
        compiler_params=pltpu.CompilerParams(vmem_limit_bytes=16 * 1024 * 1024),
    )(*gathered, norm)
    return (*finals, serve_norm.reshape(-1))


def solution(mesh):
    placed = (
        P(("trial", "zero"), "model"),
        P(("trial", "zero"), None),
        P("trial", "model"),
        P(("trial", "zero"), "model"),
        P(("trial", "zero"), None),
        P("trial", "model"),
        P(("trial", "zero"), "model"),
        P(("trial", "zero"), None),
        P("trial", "model"),
        P(("trial", "model"), "zero"),
        P(("trial", "model"), None),
        P("trial", "zero"),
        P(("trial", "zero", "model")),
        P(("trial", "zero", "model")),
    )
    return jax.shard_map(
        functools.partial(shards, mesh.shape["zero"], mesh.shape["model"]),
        mesh=mesh,
        in_specs=placed,
        out_specs=(
            P("trial", "model"),
            P("trial", "model"),
            P("trial", "model"),
            P(("trial", "model"), None),
            P("trial"),
        ),
        check_vma=False,
    )
```

```python
import functools
import math

import jax
import jax.numpy as jnp
from jax import lax
from jax.experimental import pallas as pl
from jax.experimental.pallas import tpu as pltpu
from jax.sharding import PartitionSpec as P

MESH = pl.DeviceIdType.MESH
mix_rate = 2.0
piece_rows = 512
vmem_bytes = 67043328


def merge_and_gather(zeros, models, *refs):
    (w_q, low_q, high_q, w_k, low_k, high_k, w_v, low_v, high_v, w_m, low_m, high_m) = refs[:12]
    train, step = refs[12:14]
    out_q, out_k, out_v, out_m, out_n = refs[14:19]
    held = refs[19:33]
    load_sem, send_sem, recv_sem, row_send, row_recv = refs[33:]

    z = lax.axis_index("zero")
    m = lax.axis_index("model")
    has_right, has_left = z < zeros - 1, z > 0

    barrier = pltpu.get_barrier_semaphore()

    @pl.when(has_right)
    def _():
        pl.semaphore_signal(barrier, inc=1, device_id={"zero": z + 1}, device_id_type=MESH)

    @pl.when(has_left)
    def _():
        pl.semaphore_signal(barrier, inc=1, device_id={"zero": z - 1}, device_id_type=MESH)

    for d in range(1, models):
        pl.semaphore_signal(
            barrier, inc=1, device_id={"model": lax.rem(m + d, models)}, device_id_type=MESH
        )

    loads = []
    for i in (1, 2, 0, 12, 13, 4, 5, 3, 7, 8, 6, 10, 11, 9):
        copy = pltpu.make_async_copy(refs[i], held[i], load_sem.at[i])
        copy.start()
        loads.append((i, copy))
    loads = dict(loads)

    pieces = []

    def rows_of(out, w):
        rows = w.shape[0]
        size = min(piece_rows, rows)
        return [(out, w, first, size) for first in range(0, rows, size)]

    groups = []
    for position, (out, w) in enumerate(((out_q, w_q), (out_k, w_k), (out_v, w_v), (out_m, w_m))):
        own = rows_of(out, w)
        groups.append((position, len(pieces), own))
        pieces += own
    count = len(pieces) + 1

    def view(shard, c):
        if c == count - 1:
            return out_n.at[shard]
        out, w, first, size = pieces[c]
        rows, columns = w.shape
        if out is out_m:
            return out.at[pl.ds(first, size), pl.ds(pl.multiple_of(shard * columns, columns), columns)]
        return out.at[pl.ds(pl.multiple_of(shard * rows + first, size), size), :]

    def hop(shard, c, way):
        return pltpu.make_async_remote_copy(
            src_ref=view(shard, c),
            dst_ref=view(shard, c),
            send_sem=send_sem.at[way, shard, c],
            recv_sem=recv_sem.at[shard, c],
            device_id={"zero": z + 1 if way == 0 else z - 1},
            device_id_type=MESH,
        )

    def send_own(c):
        @pl.when(has_right)
        def _():
            hop(z, c, 0).start()

        @pl.when(has_left)
        def _():
            hop(z, c, 1).start()

    def row(d):
        return pltpu.make_async_remote_copy(
            src_ref=out_n.at[z, m],
            dst_ref=out_n.at[z, m],
            send_sem=row_send.at[d],
            recv_sem=row_recv.at[d],
            device_id={"model": lax.rem(m + d, models)},
            device_id_type=MESH,
        )

    def row_from(d):
        sender = lax.rem(m + models - d, models)
        return pltpu.make_async_remote_copy(
            src_ref=out_n.at[z, sender],
            dst_ref=out_n.at[z, sender],
            send_sem=row_send.at[d],
            recv_sem=row_recv.at[d],
            device_id={"model": sender},
            device_id_type=MESH,
        )

    ready = []
    for position, base, own in groups:
        for i in (1, 2, 0):
            loads[3 * position + i].wait()
        w, low, high = held[3 * position : 3 * position + 3]
        for j, (out, _, first, size) in enumerate(own):
            product = lax.dot_general(
                low[:, first : first + size],
                high[...],
                (((0,), (0,)), ((), ())),
                preferred_element_type=jnp.float32,
            )
            merged = w[first : first + size, :].astype(jnp.float32) + mix_rate * product
            view(z, base + j)[...] = merged.astype(out.dtype)
            ready.append(base + j)
            if len(ready) == 2:
                if ready[0] == 0:
                    pl.semaphore_wait(
                        barrier, models - 1 + has_right.astype(jnp.int32) + has_left.astype(jnp.int32)
                    )
                send_own(ready.pop(0))
        if position == 0:
            loads[12].wait()
            loads[13].wait()
            out_n[z, m] = held[12][...] + held[13][...]
    for d in range(1, models):
        row(d).start()
    send_own(ready.pop(0))
    for d in range(1, models):
        row_from(d).wait_recv()
    send_own(count - 1)

    def pass_on(k, carry):
        from_left, from_right = z - 1 - k, z + 1 + k
        for c in range(count):

            @pl.when(from_left >= 0)
            def _():
                hop(from_left, c, 0).wait_recv()

                @pl.when(has_right)
                def _():
                    hop(from_left, c, 0).start()

            @pl.when(from_right < zeros)
            def _():
                hop(from_right, c, 1).wait_recv()

                @pl.when(has_left)
                def _():
                    hop(from_right, c, 1).start()

        return carry

    lax.fori_loop(0, zeros - 1, pass_on, 0)

    for d in range(1, models):
        row(d).wait_send()

    def drain(k, carry):
        for c in range(count):

            @pl.when(jnp.logical_and(has_right, z - k >= 0))
            def _():
                hop(z - k, c, 0).wait_send()

            @pl.when(jnp.logical_and(has_left, z + k < zeros))
            def _():
                hop(z + k, c, 1).wait_send()

        return carry

    lax.fori_loop(0, zeros, drain, 0)


def write_out(*refs):
    norm, wide, narrow, sem = refs[4], refs[10], refs[11], refs[12]
    copies = [pltpu.make_async_copy(refs[i], refs[5 + i], sem.at[i]) for i in (0, 3, 1, 2)]
    for copy in copies:
        copy.start()
    models = norm.shape[1]
    for i in range(wide.shape[0]):
        wide[i : i + 1, :] = norm[i // models, i % models]
    narrow[...] = wide[...].astype(narrow.dtype)
    copies.append(pltpu.make_async_copy(narrow, refs[9], sem.at[4]))
    copies[-1].start()
    for copy in copies:
        copy.wait()


def shards(zeros, models, *args):
    args = list(args)
    for i in (1, 4, 7, 10):
        args[i] = args[i].T
    for i in (12, 13):
        args[i] = args[i].reshape(1, -1)
    w_q, w_k, w_v, w_m = args[0], args[3], args[6], args[9]
    count = sum(-(-w.shape[0] // min(piece_rows, w.shape[0])) for w in (w_q, w_k, w_v, w_m)) + 1
    outs = [pltpu.VMEM((zeros * w.shape[0], w.shape[1]), w.dtype) for w in (w_q, w_k, w_v)]
    outs.append(pltpu.VMEM((w_m.shape[0], zeros * w_m.shape[1]), w_m.dtype))
    outs.append(pltpu.VMEM((zeros, models, 1, args[12].shape[1]), jnp.float32))
    held_bytes = sum(math.prod(o.shape) * jnp.dtype(o.dtype).itemsize for o in outs)
    final_query, final_key, final_value, final_mixed, norm = pl.pallas_call(
        functools.partial(merge_and_gather, zeros, models),
        out_shape=outs,
        in_specs=[pl.BlockSpec(memory_space=pltpu.HBM)] * 14,
        scratch_shapes=[pltpu.VMEM(a.shape, a.dtype) for a in args]
        + [
            pltpu.SemaphoreType.DMA((14,)),
            pltpu.SemaphoreType.DMA((2, zeros, count)),
            pltpu.SemaphoreType.DMA((zeros, count)),
            pltpu.SemaphoreType.DMA((models,)),
            pltpu.SemaphoreType.DMA((models,)),
        ],
        compiler_params=pltpu.CompilerParams(
            collective_id=0,
            has_side_effects=True,
            vmem_limit_bytes=vmem_bytes - held_bytes - 128 * 1024,
        ),
    )(*args)
    gathered = [final_query, final_key, final_value, final_mixed]
    gains = norm.shape[0] * norm.shape[1], norm.shape[3]
    *finals, serve_norm = pl.pallas_call(
        write_out,
        out_shape=[jax.ShapeDtypeStruct(g.shape, g.dtype) for g in gathered]
        + [jax.ShapeDtypeStruct(gains, jnp.bfloat16)],
        in_specs=[pl.BlockSpec(memory_space=pltpu.VMEM)] * 5,
        out_specs=[pl.BlockSpec(memory_space=pltpu.HBM)] * 5,
        scratch_shapes=[
            pltpu.VMEM(gains, jnp.float32),
            pltpu.VMEM(gains, jnp.bfloat16),
            pltpu.SemaphoreType.DMA((5,)),
        ],
        compiler_params=pltpu.CompilerParams(vmem_limit_bytes=16 * 1024 * 1024),
    )(*gathered, norm)
    return (*finals, serve_norm.reshape(-1))


def solution(mesh):
    placed = (
        P(("trial", "zero"), "model"),
        P(("trial", "zero"), None),
        P("trial", "model"),
        P(("trial", "zero"), "model"),
        P(("trial", "zero"), None),
        P("trial", "model"),
        P(("trial", "zero"), "model"),
        P(("trial", "zero"), None),
        P("trial", "model"),
        P(("trial", "model"), "zero"),
        P(("trial", "model"), None),
        P("trial", "zero"),
        P(("trial", "zero", "model")),
        P(("trial", "zero", "model")),
    )
    return jax.shard_map(
        functools.partial(shards, mesh.shape["zero"], mesh.shape["model"]),
        mesh=mesh,
        in_specs=placed,
        out_specs=(
            P("trial", "model"),
            P("trial", "model"),
            P("trial", "model"),
            P(("trial", "model"), None),
            P("trial"),
        ),
        check_vma=False,
    )
```

```python
import functools
import math

import jax
import jax.numpy as jnp
from jax import lax
from jax.experimental import pallas as pl
from jax.experimental.pallas import tpu as pltpu
from jax.sharding import PartitionSpec as P

MESH = pl.DeviceIdType.MESH
mix_rate = 2.0
piece_rows = 512
vmem_bytes = 67043328


def merge_and_gather(zeros, models, *refs):
    (w_q, low_q, high_q, w_k, low_k, high_k, w_v, low_v, high_v, w_m, low_m, high_m) = refs[:12]
    train, step = refs[12:14]
    out_q, out_k, out_v, out_m, out_n = refs[14:19]
    held = refs[19:33]
    load_sem, send_sem, recv_sem, row_send, row_recv, right_in, left_send, rows = refs[33:]

    z = lax.axis_index("zero")
    m = lax.axis_index("model")
    has_right, has_left = z < zeros - 1, z > 0

    barrier = pltpu.get_barrier_semaphore()

    @pl.when(has_right)
    def _():
        pl.semaphore_signal(barrier, inc=1, device_id={"zero": z + 1}, device_id_type=MESH)

    @pl.when(z == 0)
    def _():
        for d in range(1, models):
            pl.semaphore_signal(
                barrier, inc=1, device_id={"model": lax.rem(m + d, models)}, device_id_type=MESH
            )

    loads = []
    for i in (1, 2, 0, 12, 13, 4, 5, 3, 7, 8, 6, 10, 11, 9):
        copy = pltpu.make_async_copy(refs[i], held[i], load_sem.at[i])
        copy.start()
        loads.append((i, copy))
    loads = dict(loads)

    pieces = []

    def rows_of(out, w):
        rows = w.shape[0]
        size = min(piece_rows, rows)
        if out is out_q and rows > 128:
            return [(out, w, 0, 128), (out, w, 128, rows - 128)]
        return [(out, w, first, size) for first in range(0, rows, size)]

    groups = []
    for position, (out, w) in enumerate(((out_q, w_q), (out_k, w_k), (out_v, w_v), (out_m, w_m))):
        own = rows_of(out, w)
        groups.append((position, len(pieces), own))
        pieces += own
    count = len(pieces)

    def view(shard, c):
        out, w, first, size = pieces[c]
        rows, columns = w.shape
        if out is out_m:
            return out.at[pl.ds(first, size), pl.ds(pl.multiple_of(shard * columns, columns), columns)]
        return out.at[pl.ds(pl.multiple_of(shard * rows + first, 128), size), :]

    def hop(shard, c, way):
        return pltpu.make_async_remote_copy(
            src_ref=view(shard, c),
            dst_ref=view(shard, c),
            send_sem=send_sem.at[way, shard, c],
            recv_sem=recv_sem.at[shard, c],
            device_id={"zero": z + 1 if way == 0 else z - 1},
            device_id_type=MESH,
        )

    def send_own(c):
        @pl.when(has_left)
        def _():
            hop(z, c, 1).start()

        @pl.when(has_right)
        def _():
            if c == 0:
                pl.semaphore_wait(right_in, 1)
            hop(z, c, 0).start()

    def row_left(shard):
        return pltpu.make_async_remote_copy(
            src_ref=rows.at[shard],
            dst_ref=rows.at[shard],
            send_sem=left_send.at[0, shard],
            recv_sem=left_send.at[1, shard],
            device_id={"zero": z - 1},
            device_id_type=MESH,
        )

    def column(d, sender):
        return pltpu.make_async_remote_copy(
            src_ref=out_n.at[:, sender],
            dst_ref=out_n.at[:, sender],
            send_sem=row_send.at[d],
            recv_sem=row_recv.at[d],
            device_id={"model": lax.rem(m + d, models)},
            device_id_type=MESH,
        )

    def norm_right():
        return pltpu.make_async_remote_copy(
            src_ref=out_n,
            dst_ref=out_n,
            send_sem=row_send.at[0],
            recv_sem=row_recv.at[0],
            device_id={"zero": z + 1},
            device_id_type=MESH,
        )

    @pl.when(has_left)
    def _():
        pl.semaphore_wait(barrier, 1)
        pl.semaphore_signal(right_in, inc=1, device_id={"zero": z - 1}, device_id_type=MESH)

    ready = []
    for position, base, own in groups:
        for i in (1, 2, 0):
            loads[3 * position + i].wait()
        w, low, high = held[3 * position : 3 * position + 3]
        for j, (out, _, first, size) in enumerate(own):
            product = lax.dot_general(
                low[:, first : first + size],
                high[...],
                (((0,), (0,)), ((), ())),
                preferred_element_type=jnp.float32,
            )
            merged = w[first : first + size, :].astype(jnp.float32) + mix_rate * product
            view(z, base + j)[...] = merged.astype(out.dtype)
            ready.append(base + j)
            if len(ready) == (2 if base + j != 0 else 1):
                send_own(ready.pop(0))
        if position == 0:
            loads[12].wait()
            loads[13].wait()
            rows[z] = held[12][...] + held[13][...]

            @pl.when(has_left)
            def _():
                row_left(z).start()
    send_own(ready.pop(0))

    def pass_on(k, carry):
        from_left, from_right = z - 1 - k, z + 1 + k

        @pl.when(from_right < zeros)
        def _():
            row_left(from_right).wait_recv()

            @pl.when(has_left)
            def _():
                row_left(from_right).start()

        @pl.when(jnp.logical_and(z == 0, k == zeros - 2))
        def _():
            for i in range(zeros):
                out_n[i, m] = rows[i]
            pl.semaphore_wait(barrier, models - 1)
            for d in range(1, models):
                column(d, m).start()
            for d in range(1, models):
                column(d, lax.rem(m + models - d, models)).wait_recv()
            for d in range(1, models):
                column(d, m).wait_send()
            norm_right().start()

        for c in range(count):

            @pl.when(from_left >= 0)
            def _():
                hop(from_left, c, 0).wait_recv()

                @pl.when(has_right)
                def _():
                    hop(from_left, c, 0).start()

            @pl.when(from_right < zeros)
            def _():
                hop(from_right, c, 1).wait_recv()

                @pl.when(has_left)
                def _():
                    hop(from_right, c, 1).start()

        return carry

    lax.fori_loop(0, zeros - 1, pass_on, 0)

    @pl.when(has_left)
    def _():
        norm_right().wait_recv()

        @pl.when(has_right)
        def _():
            norm_right().start()

    @pl.when(has_right)
    def _():
        norm_right().wait_send()


    def drain(k, carry):
        @pl.when(jnp.logical_and(has_left, z + k < zeros))
        def _():
            row_left(z + k).wait_send()

        for c in range(count):

            @pl.when(jnp.logical_and(has_right, z - k >= 0))
            def _():
                hop(z - k, c, 0).wait_send()

            @pl.when(jnp.logical_and(has_left, z + k < zeros))
            def _():
                hop(z + k, c, 1).wait_send()

        return carry

    lax.fori_loop(0, zeros, drain, 0)


def write_out(*refs):
    norm, wide, narrow, sem = refs[4], refs[10], refs[11], refs[12]
    copies = [pltpu.make_async_copy(refs[i], refs[5 + i], sem.at[i]) for i in (0, 3, 1, 2)]
    for copy in copies:
        copy.start()
    models = norm.shape[1]
    for i in range(wide.shape[0]):
        wide[i : i + 1, :] = norm[i // models, i % models]
    narrow[...] = wide[...].astype(narrow.dtype)
    copies.append(pltpu.make_async_copy(narrow, refs[9], sem.at[4]))
    copies[-1].start()
    for copy in copies:
        copy.wait()


def shards(zeros, models, *args):
    args = list(args)
    for i in (1, 4, 7, 10):
        args[i] = args[i].T
    for i in (12, 13):
        args[i] = args[i].reshape(1, -1)
    w_q, w_k, w_v, w_m = args[0], args[3], args[6], args[9]
    count = sum(-(-w.shape[0] // min(piece_rows, w.shape[0])) for w in (w_q, w_k, w_v, w_m)) + 1
    outs = [pltpu.VMEM((zeros * w.shape[0], w.shape[1]), w.dtype) for w in (w_q, w_k, w_v)]
    outs.append(pltpu.VMEM((w_m.shape[0], zeros * w_m.shape[1]), w_m.dtype))
    outs.append(pltpu.VMEM((zeros, models, 1, args[12].shape[1]), jnp.float32))
    held_bytes = sum(math.prod(o.shape) * jnp.dtype(o.dtype).itemsize for o in outs)
    final_query, final_key, final_value, final_mixed, norm = pl.pallas_call(
        functools.partial(merge_and_gather, zeros, models),
        out_shape=outs,
        in_specs=[pl.BlockSpec(memory_space=pltpu.HBM)] * 14,
        scratch_shapes=[pltpu.VMEM(a.shape, a.dtype) for a in args]
        + [
            pltpu.SemaphoreType.DMA((14,)),
            pltpu.SemaphoreType.DMA((2, zeros, count)),
            pltpu.SemaphoreType.DMA((zeros, count)),
            pltpu.SemaphoreType.DMA((models,)),
            pltpu.SemaphoreType.DMA((models,)),
            pltpu.SemaphoreType.REGULAR,
            pltpu.SemaphoreType.DMA((2, zeros)),
            pltpu.VMEM((zeros, 1, args[12].shape[1]), jnp.float32),
        ],
        compiler_params=pltpu.CompilerParams(
            collective_id=0,
            has_side_effects=True,
            vmem_limit_bytes=vmem_bytes - held_bytes - 128 * 1024,
        ),
    )(*args)
    gathered = [final_query, final_key, final_value, final_mixed]
    gains = norm.shape[0] * norm.shape[1], norm.shape[3]
    *finals, serve_norm = pl.pallas_call(
        write_out,
        out_shape=[jax.ShapeDtypeStruct(g.shape, g.dtype) for g in gathered]
        + [jax.ShapeDtypeStruct(gains, jnp.bfloat16)],
        in_specs=[pl.BlockSpec(memory_space=pltpu.VMEM)] * 5,
        out_specs=[pl.BlockSpec(memory_space=pltpu.HBM)] * 5,
        scratch_shapes=[
            pltpu.VMEM(gains, jnp.float32),
            pltpu.VMEM(gains, jnp.bfloat16),
            pltpu.SemaphoreType.DMA((5,)),
        ],
        compiler_params=pltpu.CompilerParams(vmem_limit_bytes=16 * 1024 * 1024),
    )(*gathered, norm)
    return (*finals, serve_norm.reshape(-1))


def solution(mesh):
    placed = (
        P(("trial", "zero"), "model"),
        P(("trial", "zero"), None),
        P("trial", "model"),
        P(("trial", "zero"), "model"),
        P(("trial", "zero"), None),
        P("trial", "model"),
        P(("trial", "zero"), "model"),
        P(("trial", "zero"), None),
        P("trial", "model"),
        P(("trial", "model"), "zero"),
        P(("trial", "model"), None),
        P("trial", "zero"),
        P(("trial", "zero", "model")),
        P(("trial", "zero", "model")),
    )
    return jax.shard_map(
        functools.partial(shards, mesh.shape["zero"], mesh.shape["model"]),
        mesh=mesh,
        in_specs=placed,
        out_specs=(
            P("trial", "model"),
            P("trial", "model"),
            P("trial", "model"),
            P(("trial", "model"), None),
            P("trial"),
        ),
        check_vma=False,
    )
```

```python
import functools
import math

import jax
import jax.numpy as jnp
from jax import lax
from jax.experimental import pallas as pl
from jax.experimental.pallas import tpu as pltpu
from jax.sharding import PartitionSpec as P

MESH = pl.DeviceIdType.MESH
mix_rate = 2.0
piece_rows = 512
vmem_bytes = 67043328


def merge_and_gather(zeros, models, *refs):
    (w_q, low_q, high_q, w_k, low_k, high_k, w_v, low_v, high_v, w_m, low_m, high_m) = refs[:12]
    train, step = refs[12:14]
    out_q, out_k, out_v, out_m, out_n = refs[14:19]
    held = refs[19:33]
    load_sem, send_sem, recv_sem, row_send, row_recv, right_in, left_send, rows = refs[33:]

    z = lax.axis_index("zero")
    m = lax.axis_index("model")
    has_right, has_left = z < zeros - 1, z > 0

    barrier = pltpu.get_barrier_semaphore()

    @pl.when(has_right)
    def _():
        pl.semaphore_signal(barrier, inc=1, device_id={"zero": z + 1}, device_id_type=MESH)

    @pl.when(z == 0)
    def _():
        for d in range(1, models):
            pl.semaphore_signal(
                barrier, inc=1, device_id={"model": lax.rem(m + d, models)}, device_id_type=MESH
            )

    loads = []
    for i in (4, 5, 3, 1, 2, 0, 12, 13, 7, 8, 6, 10, 11, 9):
        copy = pltpu.make_async_copy(refs[i], held[i], load_sem.at[i])
        copy.start()
        loads.append((i, copy))
    loads = dict(loads)

    pieces = []

    def rows_of(out, w):
        rows = w.shape[0]
        size = min(piece_rows, rows)
        return [(out, w, first, size) for first in range(0, rows, size)]

    groups = []
    for position, out, w in ((1, out_k, w_k), (0, out_q, w_q), (2, out_v, w_v), (3, out_m, w_m)):
        own = rows_of(out, w)
        groups.append((position, len(pieces), own))
        pieces += own
    count = len(pieces)

    def view(shard, c):
        out, w, first, size = pieces[c]
        rows, columns = w.shape
        if out is out_m:
            return out.at[pl.ds(first, size), pl.ds(pl.multiple_of(shard * columns, columns), columns)]
        return out.at[pl.ds(pl.multiple_of(shard * rows + first, 128), size), :]

    def hop(shard, c, way):
        return pltpu.make_async_remote_copy(
            src_ref=view(shard, c),
            dst_ref=view(shard, c),
            send_sem=send_sem.at[way, shard, c],
            recv_sem=recv_sem.at[shard, c],
            device_id={"zero": z + 1 if way == 0 else z - 1},
            device_id_type=MESH,
        )

    def send_own(c):
        @pl.when(has_left)
        def _():
            hop(z, c, 1).start()

        @pl.when(has_right)
        def _():
            if c == 0:
                pl.semaphore_wait(right_in, 1)
            hop(z, c, 0).start()

    def row_left(shard):
        return pltpu.make_async_remote_copy(
            src_ref=rows.at[shard],
            dst_ref=rows.at[shard],
            send_sem=left_send.at[0, shard],
            recv_sem=left_send.at[1, shard],
            device_id={"zero": z - 1},
            device_id_type=MESH,
        )

    def column(d, sender):
        return pltpu.make_async_remote_copy(
            src_ref=out_n.at[:, sender],
            dst_ref=out_n.at[:, sender],
            send_sem=row_send.at[d],
            recv_sem=row_recv.at[d],
            device_id={"model": lax.rem(m + d, models)},
            device_id_type=MESH,
        )

    def norm_right():
        return pltpu.make_async_remote_copy(
            src_ref=out_n,
            dst_ref=out_n,
            send_sem=row_send.at[0],
            recv_sem=row_recv.at[0],
            device_id={"zero": z + 1},
            device_id_type=MESH,
        )

    @pl.when(has_left)
    def _():
        pl.semaphore_wait(barrier, 1)
        pl.semaphore_signal(right_in, inc=1, device_id={"zero": z - 1}, device_id_type=MESH)

    ready = []
    for position, base, own in groups:
        for i in (1, 2, 0):
            loads[3 * position + i].wait()
        w, low, high = held[3 * position : 3 * position + 3]
        for j, (out, _, first, size) in enumerate(own):
            product = lax.dot_general(
                low[:, first : first + size],
                high[...],
                (((0,), (0,)), ((), ())),
                preferred_element_type=jnp.float32,
            )
            merged = w[first : first + size, :].astype(jnp.float32) + mix_rate * product
            view(z, base + j)[...] = merged.astype(out.dtype)
            ready.append(base + j)
            if len(ready) == (2 if base + j != 0 else 1):
                send_own(ready.pop(0))
        if position == 0:
            loads[12].wait()
            loads[13].wait()
            rows[z] = held[12][...] + held[13][...]

            @pl.when(has_left)
            def _():
                row_left(z).start()
    send_own(ready.pop(0))

    def pass_on(k, carry):
        from_left, from_right = z - 1 - k, z + 1 + k

        @pl.when(from_right < zeros)
        def _():
            row_left(from_right).wait_recv()

            @pl.when(has_left)
            def _():
                row_left(from_right).start()

        @pl.when(jnp.logical_and(z == 0, k == zeros - 2))
        def _():
            for i in range(zeros):
                out_n[i, m] = rows[i]
            pl.semaphore_wait(barrier, models - 1)
            for d in range(1, models):
                column(d, m).start()
            for d in range(1, models):
                column(d, lax.rem(m + models - d, models)).wait_recv()
            for d in range(1, models):
                column(d, m).wait_send()
            norm_right().start()

        for c in range(count):

            @pl.when(from_left >= 0)
            def _():
                hop(from_left, c, 0).wait_recv()

                @pl.when(has_right)
                def _():
                    hop(from_left, c, 0).start()

            @pl.when(from_right < zeros)
            def _():
                hop(from_right, c, 1).wait_recv()

                @pl.when(has_left)
                def _():
                    hop(from_right, c, 1).start()

        return carry

    lax.fori_loop(0, zeros - 1, pass_on, 0)

    @pl.when(has_left)
    def _():
        norm_right().wait_recv()

        @pl.when(has_right)
        def _():
            norm_right().start()

    @pl.when(has_right)
    def _():
        norm_right().wait_send()


    def drain(k, carry):
        @pl.when(jnp.logical_and(has_left, z + k < zeros))
        def _():
            row_left(z + k).wait_send()

        for c in range(count):

            @pl.when(jnp.logical_and(has_right, z - k >= 0))
            def _():
                hop(z - k, c, 0).wait_send()

            @pl.when(jnp.logical_and(has_left, z + k < zeros))
            def _():
                hop(z + k, c, 1).wait_send()

        return carry

    lax.fori_loop(0, zeros, drain, 0)


def write_out(*refs):
    norm, wide, narrow, sem = refs[4], refs[10], refs[11], refs[12]
    copies = [pltpu.make_async_copy(refs[i], refs[5 + i], sem.at[i]) for i in (0, 3, 1, 2)]
    for copy in copies:
        copy.start()
    models = norm.shape[1]
    for i in range(wide.shape[0]):
        wide[i : i + 1, :] = norm[i // models, i % models]
    narrow[...] = wide[...].astype(narrow.dtype)
    copies.append(pltpu.make_async_copy(narrow, refs[9], sem.at[4]))
    copies[-1].start()
    for copy in copies:
        copy.wait()


def shards(zeros, models, *args):
    args = list(args)
    for i in (1, 4, 7, 10):
        args[i] = args[i].T
    for i in (12, 13):
        args[i] = args[i].reshape(1, -1)
    w_q, w_k, w_v, w_m = args[0], args[3], args[6], args[9]
    count = sum(-(-w.shape[0] // min(piece_rows, w.shape[0])) for w in (w_q, w_k, w_v, w_m))
    outs = [pltpu.VMEM((zeros * w.shape[0], w.shape[1]), w.dtype) for w in (w_q, w_k, w_v)]
    outs.append(pltpu.VMEM((w_m.shape[0], zeros * w_m.shape[1]), w_m.dtype))
    outs.append(pltpu.VMEM((zeros, models, 1, args[12].shape[1]), jnp.float32))
    held_bytes = sum(math.prod(o.shape) * jnp.dtype(o.dtype).itemsize for o in outs)
    final_query, final_key, final_value, final_mixed, norm = pl.pallas_call(
        functools.partial(merge_and_gather, zeros, models),
        out_shape=outs,
        in_specs=[pl.BlockSpec(memory_space=pltpu.HBM)] * 14,
        scratch_shapes=[pltpu.VMEM(a.shape, a.dtype) for a in args]
        + [
            pltpu.SemaphoreType.DMA((14,)),
            pltpu.SemaphoreType.DMA((2, zeros, count)),
            pltpu.SemaphoreType.DMA((zeros, count)),
            pltpu.SemaphoreType.DMA((models,)),
            pltpu.SemaphoreType.DMA((models,)),
            pltpu.SemaphoreType.REGULAR,
            pltpu.SemaphoreType.DMA((2, zeros)),
            pltpu.VMEM((zeros, 1, args[12].shape[1]), jnp.float32),
        ],
        compiler_params=pltpu.CompilerParams(
            collective_id=0,
            has_side_effects=True,
            vmem_limit_bytes=vmem_bytes - held_bytes - 128 * 1024,
        ),
    )(*args)
    gathered = [final_query, final_key, final_value, final_mixed]
    gains = norm.shape[0] * norm.shape[1], norm.shape[3]
    *finals, serve_norm = pl.pallas_call(
        write_out,
        out_shape=[jax.ShapeDtypeStruct(g.shape, g.dtype) for g in gathered]
        + [jax.ShapeDtypeStruct(gains, jnp.bfloat16)],
        in_specs=[pl.BlockSpec(memory_space=pltpu.VMEM)] * 5,
        out_specs=[pl.BlockSpec(memory_space=pltpu.HBM)] * 5,
        scratch_shapes=[
            pltpu.VMEM(gains, jnp.float32),
            pltpu.VMEM(gains, jnp.bfloat16),
            pltpu.SemaphoreType.DMA((5,)),
        ],
        compiler_params=pltpu.CompilerParams(vmem_limit_bytes=16 * 1024 * 1024),
    )(*gathered, norm)
    return (*finals, serve_norm.reshape(-1))


def solution(mesh):
    placed = (
        P(("trial", "zero"), "model"),
        P(("trial", "zero"), None),
        P("trial", "model"),
        P(("trial", "zero"), "model"),
        P(("trial", "zero"), None),
        P("trial", "model"),
        P(("trial", "zero"), "model"),
        P(("trial", "zero"), None),
        P("trial", "model"),
        P(("trial", "model"), "zero"),
        P(("trial", "model"), None),
        P("trial", "zero"),
        P(("trial", "zero", "model")),
        P(("trial", "zero", "model")),
    )
    return jax.shard_map(
        functools.partial(shards, mesh.shape["zero"], mesh.shape["model"]),
        mesh=mesh,
        in_specs=placed,
        out_specs=(
            P("trial", "model"),
            P("trial", "model"),
            P("trial", "model"),
            P(("trial", "model"), None),
            P("trial"),
        ),
        check_vma=False,
    )
```
